32 devices in a mesh: gx: 8 (over y, x, core), gy: 4 (over z).
Axes of the slice: x: 2, y: 2, z: 4, core: 2. Of those that a mesh axis runs over, the one named last changes fastest.
Arguments:
- obstacles: int32 [1024, 1024], P('gx', 'gy'), may hold values 0 or 1
- load: float32 [1024, 1024], P('gx', 'gy'), may hold values from 0.25 to 4
- exit_rows: int32 [4, 256], replicated, may hold values from 0 to 1023
- exit_cols: int32 [4, 256], replicated, may hold values from 0 to 1023
Outputs:
- potential: float32 [4, 1024, 1024], P(None, 'gx', 'gy')
The draws below stay inside these ranges and needn't reach their ends.
All inputs are finite; a program needn't handle non-finite values. No bound on the sum of `obstacles` on one device may be relied on, other than what follows from the above.
Results may differ from the reference program's by a relative error of at most 0.0001.
Values sent between devices are 32-bit elements; how exact they have to be, the bound alone decides.
A program may use at most 64 MiB of HBM per device.

```python
import jax
import jax.numpy as jnp

GOALS = 4
COARSEN = 4
SMOOTH = 4
CSWEEPS = 4
CYCLES = 2
NX = 1024
NY = 1024
EXITS = 256


def draw_load(key, part):
    rough_part = jax.random.uniform(key, (NX, NY), jnp.float32, 0.25, 2.0)
    return rough_part


def touch_ends(values, own_key, smallest, largest):
    index_at = [jax.random.randint(jax.random.fold_in(own_key, axis), (), 0, length) for axis, length in enumerate(values.shape)]
    main_axis = values.shape.index(max(values.shape))
    beside = index_at[:main_axis] + [(index_at[main_axis] + 1) % values.shape[main_axis]] + index_at[main_axis + 1:]
    return values.at[tuple(index_at)].set(smallest).at[tuple(beside)].set(largest)


def setup_inputs(seed: int = 0) -> dict:
    key_of = jax.random.split(jax.random.key(seed), 5)
    return {
        "obstacles": touch_ends((jax.random.randint(key_of[0], (NX, NY), 0, 5) < 1).astype(jnp.int32), jax.random.fold_in(key_of[0], 1), 0, 1),
        "load": draw_load(jax.random.fold_in(key_of[4], 71), 0),
        "exit_rows": touch_ends(jax.random.randint(key_of[2], (GOALS, EXITS), 0, NX), jax.random.fold_in(key_of[2], 1), 0, NX - 1).astype(jnp.int32),
        "exit_cols": touch_ends(jax.random.randint(key_of[3], (GOALS, EXITS), 0, NY), jax.random.fold_in(key_of[3], 1), 0, NY - 1).astype(jnp.int32),
    }


SCREENING = 1e-4
EXIT_SINK = 4.0
COARSE_SHIFT = 0.01
DAMPING = 0.8
UPPER_BOUND = 12.5
LOWER_BOUND = 1.0


def cross_sum(field):
    padded = jnp.pad(field, ((0, 0), (1, 1), (1, 1)))
    return padded[:, 2:, 1:-1] + padded[:, :-2, 1:-1] + padded[:, 1:-1, 2:] + padded[:, 1:-1, :-2]


def chebyshev(start, residual, operate):
    center = 0.5 * (UPPER_BOUND + LOWER_BOUND)
    half_span = 0.5 * (UPPER_BOUND - LOWER_BOUND)
    sigma_ratio = center / half_span
    ratio_old = 1.0 / sigma_ratio
    update = residual / center
    result = start + update
    for sweep in range(SMOOTH - 1):
        residual = residual - operate(update)
        ratio_new = 1.0 / (2.0 * sigma_ratio - ratio_old)
        update = (ratio_new * ratio_old) * update + (2.0 * ratio_new / half_span) * residual
        result = result + update
        ratio_old = ratio_new
    return result


def restrict(residual):
    goals, height, width = residual.shape
    blocks = residual.reshape(goals, height // COARSEN, COARSEN, width // COARSEN, COARSEN)
    return blocks.mean(axis=(2, 4))


def coarse_solve(coarse_rhs):
    center_weight = 4.0 + COARSE_SHIFT
    estimate = DAMPING * coarse_rhs / center_weight
    for sweep in range(CSWEEPS - 1):
        estimate = estimate + DAMPING * (coarse_rhs - (center_weight * estimate - cross_sum(estimate))) / center_weight
    return estimate


def prolong(estimate, open_cells):
    expanded = jnp.repeat(jnp.repeat(estimate, COARSEN, axis=1), COARSEN, axis=2)
    return open_cells * expanded


def reference(obstacles, load, exit_rows, exit_cols):
    open_cells = (1 - obstacles).astype(jnp.float32)
    neighbours = cross_sum(open_cells[None])[0]
    goals = exit_rows.shape[0]
    flat_index = (exit_rows * NY + exit_cols).astype(jnp.int32)
    goal_index = jnp.broadcast_to(jnp.arange(goals, dtype=jnp.int32)[:, None], flat_index.shape)
    marks = jnp.zeros((goals, NX * NY), jnp.float32).at[goal_index, flat_index].add(1.0)
    exits = jnp.minimum(marks, 1.0).reshape(goals, NX, NY)
    diagonal = SCREENING + 4.0 * (1.0 - open_cells) + open_cells * neighbours + EXIT_SINK * open_cells * exits

    def operate(field):
        return diagonal * field - open_cells * cross_sum(open_cells * field)

    source = jnp.broadcast_to(open_cells * load, (goals, NX, NY))
    potential = chebyshev(jnp.zeros_like(source), source, operate)
    estimate = coarse_solve(restrict(source))
    for cycle in range(1, CYCLES):
        correction = prolong(estimate, open_cells)
        residual = source - operate(potential)
        shifted = residual - operate(correction)
        estimate_next = coarse_solve(restrict(residual))
        potential = chebyshev(potential + correction, shifted, operate)
        estimate = estimate_next
    return potential + prolong(estimate, open_cells)
```

```python
import functools

import jax
import jax.numpy as jnp
from jax import lax
from jax.experimental import pallas as pl
from jax.experimental.pallas import tpu as pltpu
from jax.sharding import PartitionSpec as P

COARSEN = 4
SMOOTH = 4
CSWEEPS = 4

SCREENING = 0.0001
EXIT_SINK = 4.0
COARSE_SHIFT = 0.01
DAMPING = 0.8
UPPER_BOUND = 12.5
LOWER_BOUND = 1.0

CENTER = 0.5 * (UPPER_BOUND + LOWER_BOUND)
LANES = 128
SUB = 8
UNROLL = 8
HALO = COARSEN * CSWEEPS
COARSE_HALO = HALO // COARSEN
RIGHT_HALO = LANES - 3 * HALO
LEFT_OWN = 3 * HALO
EDGE = HALO // SUB

DIRECTIONS = ((-1, 0), (1, 0), (0, -1), (0, 1), (-1, -1), (-1, 1), (1, -1), (1, 1))


def smoother_coefficients():
    def add(p, q):
        size = max(len(p), len(q))
        p, q = p + [0.0] * (size - len(p)), q + [0.0] * (size - len(q))
        return [a + b for a, b in zip(p, q)]

    def scale(k, p):
        return [k * a for a in p]

    half_span = 0.5 * (UPPER_BOUND - LOWER_BOUND)
    sigma_ratio = CENTER / half_span
    ratio_old = 1.0 / sigma_ratio
    residual = [1.0]
    update = scale(1.0 / CENTER, residual)
    result = update
    for sweep in range(SMOOTH - 1):
        applied = scale(CENTER, add(update, scale(-1.0, [0.0] + update)))
        residual = add(residual, scale(-1.0, applied))
        ratio_new = 1.0 / (2.0 * sigma_ratio - ratio_old)
        update = add(
            scale(ratio_new * ratio_old, update), scale(2.0 * ratio_new / half_span, residual)
        )
        result = add(result, update)
        ratio_old = ratio_new
    return result


def lane_iota(rows):
    return lax.broadcasted_iota(jnp.int32, (rows, LANES), 1)


def cycles_kernel(
    peers, obst_hbm, load_hbm, rows_hbm, cols_hbm, out_ref,
    obst_ref, load_ref, exit_rows_ref, exit_cols_ref, source_ref, open_ref, marks_ref, diag_ref,
    first_ref, second_ref, third_ref, rest_ref, shift_ref, fourth_ref, fifth_ref, corr_ref,
    inner_ref, expand_ref, last_ref,
    top, bot, lef, rig, top_corner, bot_corner, from_rows, from_cols, from_corners,
    input_sem, send_sem, recv_sem,
):
    goals, rows, cols = out_ref.shape
    tiles = cols // LANES
    rim = tiles
    span = tiles + 1
    ring = span * LANES
    wide = rows + 2 * HALO
    groups = wide // SUB
    first = SUB + HALO
    coarse_rows = wide // COARSEN
    own_coarse = rows // COARSEN
    me = (lax.axis_index("gx"), lax.axis_index("gy"))
    row_start = me[0] * rows
    col_start = me[1] * cols
    lane = lane_iota(SUB)
    sub = lax.broadcasted_iota(jnp.int32, (SUB, LANES), 0)
    zero = jnp.zeros((SUB, LANES), jnp.float32)
    coefficients = smoother_coefficients()
    inverse = 1.0 / CENTER
    natural = list(range(tiles))

    def exists(dx, dy):
        gx, gy = me[0] + dx, me[1] + dy
        return (gx >= 0) & (gx < peers[0]) & (gy >= 0) & (gy < peers[1])

    barrier = pltpu.get_barrier_semaphore()
    count = jnp.int32(0)
    for dx, dy in DIRECTIONS:
        there = exists(dx, dy)
        count = count + there.astype(jnp.int32)

        @pl.when(there)
        def _():
            pl.semaphore_signal(
                barrier, inc=1, device_id=(me[0] + dx, me[1] + dy),
                device_id_type=pl.DeviceIdType.MESH,
            )

    pairs = (
        (obst_hbm, obst_ref), (load_hbm, load_ref), (rows_hbm, exit_rows_ref),
        (cols_hbm, exit_cols_ref),
    )
    inputs = [
        pltpu.make_async_copy(there, here, input_sem.at[k]) for k, (there, here) in enumerate(pairs)
    ]
    for copied in inputs:
        copied.start()

    messages = (
        (top, from_rows.at[0]),
        (bot, from_rows.at[1]),
        (lef, from_cols.at[0]),
        (rig, from_cols.at[1]),
        (top_corner, from_corners.at[0]),
        (top.at[tiles - 1], from_corners.at[1]),
        (bot_corner, from_corners.at[2]),
        (bot.at[tiles - 1], from_corners.at[3]),
    )

    def copy(k):
        dx, dy = DIRECTIONS[k]
        return pltpu.make_async_remote_copy(
            src_ref=messages[k][0], dst_ref=messages[k][1],
            send_sem=send_sem.at[k], recv_sem=recv_sem.at[k],
            device_id=(me[0] + dx, me[1] + dy), device_id_type=pl.DeviceIdType.MESH,
        )

    def arrive(k):
        dx, dy = DIRECTIONS[k]

        @pl.when(exists(-dx, -dy))
        def _():
            copy(k).wait_recv()

    for k, (dx, dy) in enumerate(DIRECTIONS):

        @pl.when(jnp.logical_not(exists(-dx, -dy)))
        def _():
            messages[k][1][...] = jnp.zeros(messages[k][1].shape, jnp.float32)

    for ends in (0, wide + SUB):
        for t in range(span):
            open_ref[t, pl.ds(ends, SUB), :] = zero
            source_ref[t, pl.ds(ends, SUB), :] = zero
            for g in range(goals):
                for ref in (first_ref, second_ref, third_ref):
                    ref[g, t, pl.ds(ends, SUB), :] = zero

    def row(ref, at, t, *lead):
        return ref[(*lead, t, pl.ds(at, SUB), slice(None))]

    def around(ref, at, ts, *lead):
        center = [row(ref, at, t, *lead) for t in ts]
        below = [row(ref, at + 1, t, *lead) for t in ts]
        above = [row(ref, at - 1, t, *lead) for t in ts]
        up = [pltpu.roll(c, 1, 1) for c in center]
        down = [pltpu.roll(c, LANES - 1, 1) for c in center]
        total = []
        for k in range(len(ts)):
            before = jnp.where(lane == 0, up[k - 1], up[k]) if k else up[k]
            after = (
                jnp.where(lane == LANES - 1, down[k + 1], down[k]) if k + 1 < len(ts) else down[k]
            )
            total.append(below[k] + above[k] + (before + after))
        return center, total

    def inner(body):
        low, high = EDGE, groups - EDGE
        size = high - low
        unroll = max(u for u in range(1, UNROLL + 1) if size % u == 0)

        def step(i, carry):
            body(i, pl.multiple_of(i * SUB + SUB, SUB), natural)
            return carry

        lax.fori_loop(low, high, step, 0, unroll=unroll)

    def over(members, ts, body):
        for i in sorted(set(members)):
            body(i, i * SUB + SUB, ts)

    early = [*range(EDGE + 1), *range(groups - EDGE - 1, groups)]
    late = [*range(EDGE - 1, 2 * EDGE), *range(groups - 2 * EDGE, groups - EDGE + 1)]
    final = [*range(EDGE, 2 * EDGE), *range(groups - 2 * EDGE, groups - EDGE)]

    def setup(i, at, ts):
        opened, open_around = around(open_ref, at, ts)
        source, source_around = around(source_ref, at, ts)
        for k, t in enumerate(ts):
            base = (1.0 - inverse * (SCREENING + 4.0)) + opened[k] * (
                4.0 * inverse - inverse * open_around[k]
            )
            mixed = (coefficients[3] * inverse) * opened[k] * source_around[k]
            mixed = mixed + coefficients[2] * source[k]
            lifted = coefficients[3] * source[k]
            for g in range(goals):
                kept = base + opened[k] * row(marks_ref, at, t, g)
                diag_ref[g, t, pl.ds(at, SUB), :] = kept
                first_ref[g, t, pl.ds(at, SUB), :] = kept * lifted + mixed

    def horner(old_ref, new_ref, coefficient, rhs):
        def body(i, at, ts):
            weight = [inverse * row(open_ref, at, t) for t in ts]
            for g in range(goals):
                center, total = around(old_ref, at, ts, g)
                for k, t in enumerate(ts):
                    kept = row(diag_ref, at, t, g)
                    new_ref[g, t, pl.ds(at, SUB), :] = (
                        kept * center[k] + weight[k] * total[k] + coefficient * rhs(g, t, at)
                    )

        return body

    plain = lambda g, t, at: row(source_ref, at, t)
    shifted = lambda g, t, at: row(shift_ref, at, t, g)
    second = horner(first_ref, second_ref, coefficients[1], plain)
    third = horner(second_ref, third_ref, coefficients[0], plain)
    fifth = horner(fourth_ref, fifth_ref, coefficients[1], shifted)

    def residual(i, at, ts):
        opened = [row(open_ref, at, t) for t in ts]
        for g in range(goals):
            center, total = around(third_ref, at, ts, g)
            for k, t in enumerate(ts):
                kept = CENTER * (row(diag_ref, at, t, g) - 1.0)
                rest_ref[g, t, pl.ds(at, SUB), :] = (
                    row(source_ref, at, t) + kept * center[k] + opened[k] * total[k]
                )

    def spread(ref, at, t, *lead):
        even = jnp.broadcast_to(ref[(*lead, t, pl.ds(at, 1), slice(None))], (SUB, LANES))
        odd = jnp.broadcast_to(ref[(*lead, t, pl.ds(at + 1, 1), slice(None))], (SUB, LANES))
        return jnp.where(sub < COARSEN, even, odd)

    def corrections(ref, skip):
        def body(i, at, ts):
            for t in ts:
                corr_ref[t, pl.ds(at, SUB), :] = row(open_ref, at, t) * spread(ref, 2 * (i - skip), t)

        return body

    def shift(i, at, ts):
        opened = [row(open_ref, at, t) for t in ts]
        center, total = around(corr_ref, at, ts)
        moved = [opened[k] * total[k] for k in range(len(ts))]
        for g in range(goals):
            for k, t in enumerate(ts):
                kept = CENTER * (row(diag_ref, at, t, g) - 1.0)
                shift_ref[g, t, pl.ds(at, SUB), :] = (
                    row(rest_ref, at, t, g) + kept * center[k] + moved[k]
                )

    def fourth(i, at, ts):
        weight = [(coefficients[3] * inverse) * row(open_ref, at, t) for t in ts]
        for g in range(goals):
            center, total = around(shift_ref, at, ts, g)
            for k, t in enumerate(ts):
                kept = row(diag_ref, at, t, g)
                fourth_ref[g, t, pl.ds(at, SUB), :] = (
                    (coefficients[3] * kept + coefficients[2]) * center[k] + weight[k] * total[k]
                )

    def result(put):
        def body(i, at, ts):
            weight = [inverse * row(open_ref, at, t) for t in ts]
            for g in range(goals):
                center, total = around(fifth_ref, at, ts, g)
                for k, t in enumerate(ts):
                    put(
                        g, t, at - first,
                        row(third_ref, at, t, g) + row(corr_ref, at, t)
                        + row(diag_ref, at, t, g) * center[k] + weight[k] * total[k]
                        + coefficients[0] * row(shift_ref, at, t, g),
                    )

        return body

    def put(g, t, at, value):
        start = at if isinstance(at, int) else pl.multiple_of(at, SUB)
        out_ref[g, pl.ds(start, SUB), pl.ds(t * LANES, LANES)] = value

    def put_rim(g, t, at, value):
        left = (g, pl.ds(at, SUB), pl.ds(0, LANES))
        out_ref[left] = jnp.where(lane < HALO, value, out_ref[left])
        fourth_ref[g, t, pl.ds(at, SUB), :] = value

    position = lax.broadcasted_iota(jnp.int32, (ring, LANES), 0)
    rim_lane = position - cols
    fine = jnp.where(
        position < cols + LEFT_OWN,
        jnp.where(position < cols, position, rim_lane),
        jnp.where(
            rim_lane < RIGHT_HALO + HALO,
            rim_lane + (cols - RIGHT_HALO), rim_lane + (COARSEN - 1) * LANES,
        ),
    ) // COARSEN
    member = (rim_lane < RIGHT_HALO + HALO) | (rim_lane >= LANES - HALO)
    trusted = ((position >= HALO) & (position < cols - HALO)) | (
        (rim_lane >= 0) & ((rim_lane < HALO) | ((rim_lane >= RIGHT_HALO - HALO) & member))
    )
    same = fine == lax.broadcasted_iota(jnp.int32, (ring, LANES), 1)
    expands = jnp.where(same & member, 1.0, 0.0).astype(jnp.bfloat16)
    restricts = jnp.where(same & trusted, 1.0, 0.0).astype(jnp.bfloat16)

    def product(value, matrix, dims):
        high = value.astype(jnp.bfloat16)
        low = (value - high.astype(jnp.float32)).astype(jnp.bfloat16)
        both = lax.dot_general(
            jnp.concatenate([high, low], axis=0), matrix, (dims, ((), ())),
            preferred_element_type=jnp.float32,
        )
        size = value.shape[0]
        return both[:size] + both[size:]

    def restrict(ref, offset, size, ts, matrix, leads):
        stacked = []
        for t in ts:
            blocks = []
            for lead in leads:
                part = [
                    ref[(*lead, t, pl.ds(offset + k, size, stride=COARSEN), slice(None))]
                    for k in range(COARSEN)
                ]
                blocks.append((part[0] + part[1]) + (part[2] + part[3]))
            stacked.append(jnp.concatenate(blocks, axis=0) if len(blocks) > 1 else blocks[0])
        total = product(jnp.concatenate(stacked, axis=1), matrix, ((1,), (0,)))
        return total * (1.0 / (COARSEN * COARSEN))

    shape = (coarse_rows, LANES)
    coarse_row = lax.broadcasted_iota(jnp.int32, shape, 0) - COARSE_HALO + row_start // COARSEN
    coarse_lane = lax.broadcasted_iota(jnp.int32, shape, 1)
    coarse_col = (
        jnp.where(coarse_lane < cols // COARSEN + LANES // 8, coarse_lane, coarse_lane - LANES)
        + col_start // COARSEN
    )
    floor = (
        (coarse_row >= 0) & (coarse_row < peers[0] * rows // COARSEN)
        & (coarse_col >= 0) & (coarse_col < peers[1] * cols // COARSEN)
    ).astype(jnp.float32)

    def coarse_solve(rhs, inside):
        center_weight = 4.0 + COARSE_SHIFT
        gain = DAMPING / center_weight
        size = rhs.shape[0]
        scaled = gain * rhs
        estimate = scaled if inside is None else scaled * inside
        for sweep in range(CSWEEPS - 1):
            near = (
                pltpu.roll(estimate, size - 1, 0) + pltpu.roll(estimate, 1, 0)
                + pltpu.roll(estimate, LANES - 1, 1) + pltpu.roll(estimate, 1, 1)
            )
            estimate = (1.0 - DAMPING) * estimate + (scaled + gain * near)
            if inside is not None:
                estimate = estimate * inside
        return estimate

    for copied in inputs:
        copied.wait()

    def blend(i, at):
        for t in natural:
            block = (pl.ds(at, SUB), pl.ds(t * LANES, LANES))
            opened = (1 - obst_ref[block]).astype(jnp.float32)
            into = (t, pl.ds(at + first, SUB), slice(None))
            open_ref[into] = opened
            source_ref[into] = opened * load_ref[block]

    for at in range(0, rows, SUB):
        blend(at, at)

    def mixed_rim(left_tile, right_tile):
        turned = pltpu.roll(right_tile, RIGHT_HALO, 1)
        return jnp.where(lane < LEFT_OWN, left_tile, jnp.where(lane < RIGHT_HALO, turned, 0.0))

    for t in natural:
        top[t] = source_ref[t, pl.ds(first, HALO), :]
        bot[t] = source_ref[t, pl.ds(first + rows - HALO, HALO), :]
    top_corner[...] = pltpu.roll(source_ref[0, pl.ds(first, HALO), :], RIGHT_HALO, 1)
    bot_corner[...] = pltpu.roll(source_ref[0, pl.ds(first + rows - HALO, HALO), :], RIGHT_HALO, 1)
    tall = lane_iota(HALO)
    block = LANES // HALO
    for pack in range(rows // LANES):
        left = jnp.zeros((HALO, LANES), jnp.float32)
        right = jnp.zeros((HALO, LANES), jnp.float32)
        for b in range(block):
            start = first + pack * LANES + b * HALO
            here = (tall >= b * HALO) & (tall < (b + 1) * HALO)
            low = source_ref[0, pl.ds(start, HALO), :]
            high = source_ref[tiles - 1, pl.ds(start, HALO), :]
            left = jnp.where(here, pltpu.roll(low, b * HALO, 1) if b else low, left)
            turn = ((b + 1) * HALO) % LANES
            right = jnp.where(here, pltpu.roll(high, turn, 1) if turn else high, right)
        lef[pl.ds(pack * HALO, HALO), :] = left
        rig[pl.ds(pack * HALO, HALO), :] = right
    for i in range(EDGE, groups - EDGE):
        at = i * SUB + SUB
        source_ref[rim, pl.ds(at, SUB), :] = mixed_rim(
            row(source_ref, at, 0), row(source_ref, at, tiles - 1)
        )

    exits = exit_rows_ref.shape[1]
    row_of = lax.broadcasted_iota(jnp.int32, (wide, exits), 0) + (row_start - HALO)
    spot = lax.broadcasted_iota(jnp.int32, (ring, exits), 0)
    col_of = jnp.where(
        spot < cols, spot,
        jnp.where(
            spot < cols + LEFT_OWN, spot - cols,
            jnp.where(spot < cols + RIGHT_HALO + HALO, spot - RIGHT_HALO, spot - (cols + LANES)),
        ),
    ) + col_start
    for g in range(goals):
        row_hot = (row_of == exit_rows_ref[pl.ds(g, 1), :]).astype(jnp.float32)
        col_hot = (col_of == exit_cols_ref[pl.ds(g, 1), :]).astype(jnp.float32)
        marks = lax.dot_general(
            row_hot.astype(jnp.bfloat16), col_hot.astype(jnp.bfloat16),
            (((1,), (1,)), ((), ())), preferred_element_type=jnp.float32,
        )
        marks = jnp.minimum(marks, 1.0) * (-EXIT_SINK * inverse)
        for t in range(span):
            marks_ref[g, t, pl.ds(SUB, wide), :] = marks[:, t * LANES : (t + 1) * LANES]

    def part_one():
        inner(setup)
        inner(second)

    def part_two():
        inner(third)
        inner(residual)
        known = coarse_solve(
            restrict(source_ref, first, own_coarse, natural, expands[:cols], [()]), None
        )
        columns = product(known, expands[:cols], ((1,), (1,)))
        for t in natural:
            inner_ref[t] = columns[:, t * LANES : (t + 1) * LANES]
        inner(corrections(inner_ref, EDGE))
        inner(shift)
        inner(fourth)
        inner(fifth)
        inner(result(put))

    part_one()

    pl.semaphore_wait(barrier, count)
    order = (4, 5, 6, 7, 2, 3, 0, 1)
    for k in order:

        @pl.when(exists(*DIRECTIONS[k]))
        def _():
            copy(k).start()

    part_two()

    arrive(0)
    arrive(1)
    for t in natural:
        for here, ref in ((first + rows, from_rows.at[0, t]), (SUB, from_rows.at[1, t])):
            for b in range(EDGE):
                value = ref[pl.ds(b * SUB, SUB), :]
                source_ref[t, pl.ds(here + b * SUB, SUB), :] = value
                open_ref[t, pl.ds(here + b * SUB, SUB), :] = (value > 0.0).astype(jnp.float32)
    over(early, natural, setup)
    over(early, natural, second)
    over(early, natural, third)
    over(early, natural, residual)

    arrive(2)
    arrive(3)
    for k in (4, 5, 6, 7):
        arrive(k)

    is_right = (lane >= RIGHT_HALO) & (lane < RIGHT_HALO + HALO)
    is_left = lane >= LANES - HALO

    def set_rim(at, value):
        source_ref[rim, pl.ds(at, SUB), :] = value
        open_ref[rim, pl.ds(at, SUB), :] = (value > 0.0).astype(jnp.float32)

    for side, here in ((0, first + rows), (1, SUB)):
        for b in range(EDGE):
            at = here + b * SUB
            part = pl.ds(b * SUB, SUB)
            base = mixed_rim(row(source_ref, at, 0), row(source_ref, at, tiles - 1))
            value = jnp.where(is_right, from_corners[2 * side, part, :], base)
            set_rim(at, jnp.where(is_left, from_corners[2 * side + 1, part, :], value))
    for pack in range(rows // LANES):
        for b in range(block):
            for c in range(EDGE):
                part = pl.ds(pack * HALO + c * SUB, SUB)
                right = pltpu.roll(from_cols[0, part, :], (RIGHT_HALO - b * HALO) % LANES, 1)
                left = from_cols[1, part, :]
                turn = (LANES - HALO - b * HALO) % LANES
                left = pltpu.roll(left, turn, 1) if turn else left
                at = first + pack * LANES + b * HALO + c * SUB
                value = jnp.where(is_right, right, row(source_ref, at, rim))
                set_rim(at, jnp.where(is_left, left, value))

    everything = list(range(span))
    known = coarse_solve(restrict(source_ref, SUB, coarse_rows, everything, restricts, [()]), floor)
    columns = product(known, expands, ((1,), (1,)))
    for t in everything:
        expand_ref[t] = columns[:, t * LANES : (t + 1) * LANES]

    tall_rim, short_rim, own_rim = (range(k, groups - k) for k in (0, EDGE - 1, EDGE))
    over(tall_rim, [rim], setup)
    over(tall_rim, [rim], second)
    over(tall_rim, [rim], third)
    over(tall_rim, [rim], residual)

    leads = [(g,) for g in range(goals)]
    estimates = coarse_solve(
        restrict(rest_ref, SUB, coarse_rows, everything, restricts, leads),
        jnp.concatenate([floor] * goals, axis=0),
    )
    columns = product(estimates, expands[:cols], ((1,), (1,)))
    for g in range(goals):
        for t in natural:
            last_ref[g, t] = columns[
                g * coarse_rows : (g + 1) * coarse_rows, t * LANES : (t + 1) * LANES
            ]

    for ts, members in (([rim], short_rim), (natural, late)):
        over(members, ts, corrections(expand_ref, 0))
    for body in (shift, fourth, fifth):
        for ts, members in (([rim], short_rim), (natural, late)):
            over(members, ts, body)
    over(final, natural, result(put))
    over(own_rim, [rim], result(put_rim))
    for i in range(EDGE, groups - EDGE):
        at = i * SUB + SUB - first
        for g in range(goals):
            right = (g, pl.ds(at, SUB), pl.ds(cols - LANES, LANES))
            turned = pltpu.roll(row(fourth_ref, at, rim, g), LANES - RIGHT_HALO, 1)
            out_ref[right] = jnp.where(lane >= LANES - HALO, turned, out_ref[right])

    for i in range(EDGE, groups - EDGE):
        at = i * SUB + SUB
        opened = [row(open_ref, at, t) for t in natural]
        for g in range(goals):
            for t in natural:
                block = (g, pl.ds(at - first, SUB), pl.ds(t * LANES, LANES))
                out_ref[block] = out_ref[block] + opened[t] * spread(last_ref, 2 * i, t, g)

    for k in order:

        @pl.when(exists(*DIRECTIONS[k]))
        def _():
            copy(k).wait_send()


def per_device(peers, obstacles, load, exit_rows, exit_cols):
    rows, cols = obstacles.shape
    goals = exit_rows.shape[0]
    tiles = cols // LANES
    span = tiles + 1
    wide = rows + 2 * HALO
    padded = wide + 2 * SUB
    f32 = jnp.float32
    vmem = pl.BlockSpec(memory_space=pltpu.VMEM)
    packed = rows * HALO // LANES
    exits = exit_rows.shape
    field = pltpu.VMEM((goals, span, padded, LANES), f32)
    shared = pltpu.VMEM((span, padded, LANES), f32)
    coarse = wide // COARSEN
    strip = pltpu.VMEM((tiles, HALO, LANES), f32)
    column = pltpu.VMEM((packed, LANES), f32)
    corner = pltpu.VMEM((HALO, LANES), f32)
    return pl.pallas_call(
        functools.partial(cycles_kernel, peers),
        out_shape=jax.ShapeDtypeStruct((goals, rows, cols), f32),
        in_specs=[pl.BlockSpec(memory_space=pltpu.HBM)] * 4,
        out_specs=vmem,
        scratch_shapes=[
            pltpu.VMEM((rows, cols), jnp.int32),
            pltpu.VMEM((rows, cols), f32),
            pltpu.VMEM(exits, jnp.int32),
            pltpu.VMEM(exits, jnp.int32),
            shared, shared, field, field,
            field, field, field, field, field, field, field, shared,
            pltpu.VMEM((tiles, rows // COARSEN, LANES), f32),
            pltpu.VMEM((span, coarse, LANES), f32),
            pltpu.VMEM((goals, tiles, coarse, LANES), f32),
            strip, strip, column, column, corner, corner,
            pltpu.VMEM((2, tiles, HALO, LANES), f32),
            pltpu.VMEM((2, packed, LANES), f32),
            pltpu.VMEM((4, HALO, LANES), f32),
            pltpu.SemaphoreType.DMA((4,)),
            pltpu.SemaphoreType.DMA((len(DIRECTIONS),)),
            pltpu.SemaphoreType.DMA((len(DIRECTIONS),)),
        ],
        compiler_params=pltpu.CompilerParams(
            collective_id=0, has_side_effects=True, vmem_limit_bytes=48 * 1024 * 1024
        ),
        name="cycles",
    )(*(pltpu.with_memory_space_constraint(x, pltpu.HBM) for x in (obstacles, load, exit_rows, exit_cols)))


def solution(mesh):
    peers = (mesh.shape["gx"], mesh.shape["gy"])
    return jax.shard_map(
        functools.partial(per_device, peers),
        mesh=mesh,
        in_specs=(P("gx", "gy"), P("gx", "gy"), P(), P()),
        out_specs=P(None, "gx", "gy"),
        check_vma=False,
    )
```

```python
import functools
import math

import jax
import jax.numpy as jnp
from jax import lax
from jax.experimental import pallas as pl
from jax.experimental.pallas import tpu as pltpu
from jax.sharding import PartitionSpec as P

COARSEN = 4
SMOOTH = 4
CSWEEPS = 4

SCREENING = 0.0001
EXIT_SINK = 4.0
COARSE_SHIFT = 0.01
DAMPING = 0.8
UPPER_BOUND = 12.5
LOWER_BOUND = 1.0

CENTER = 0.5 * (UPPER_BOUND + LOWER_BOUND)
LANES = 128
SUB = 8
UNROLL = 16
HALO = COARSEN * CSWEEPS
COARSE_HALO = HALO // COARSEN
RIGHT_HALO = LANES - 3 * HALO
LEFT_OWN = 3 * HALO
EDGE = HALO // SUB

DIRECTIONS = ((-1, 0), (1, 0), (0, -1), (0, 1), (-1, -1), (-1, 1), (1, -1), (1, 1))


def smoother_coefficients():
    def add(p, q):
        size = max(len(p), len(q))
        p, q = p + [0.0] * (size - len(p)), q + [0.0] * (size - len(q))
        return [a + b for a, b in zip(p, q)]

    def scale(k, p):
        return [k * a for a in p]

    half_span = 0.5 * (UPPER_BOUND - LOWER_BOUND)
    sigma_ratio = CENTER / half_span
    ratio_old = 1.0 / sigma_ratio
    residual = [1.0]
    update = scale(1.0 / CENTER, residual)
    result = update
    for sweep in range(SMOOTH - 1):
        applied = scale(CENTER, add(update, scale(-1.0, [0.0] + update)))
        residual = add(residual, scale(-1.0, applied))
        ratio_new = 1.0 / (2.0 * sigma_ratio - ratio_old)
        update = add(
            scale(ratio_new * ratio_old, update), scale(2.0 * ratio_new / half_span, residual)
        )
        result = add(result, update)
        ratio_old = ratio_new
    return result


def coarse_coefficients():
    gain = DAMPING / (4.0 + COARSE_SHIFT)
    powers = [gain]
    for sweep in range(CSWEEPS - 1):
        size = len(powers)
        powers = [
            (1.0 - DAMPING) * (powers[k] if k < size else 0.0)
            + gain * (powers[k - 1] if k else 1.0)
            for k in range(size + 1)
        ]
    return [value / (COARSEN * COARSEN) for value in powers]


def lane_iota(rows):
    return lax.broadcasted_iota(jnp.int32, (rows, LANES), 1)


def cycles_kernel(
    peers, obst_hbm, load_hbm, rows_hbm, cols_hbm, out_ref,
    obst_ref, load_ref, exit_rows_ref, exit_cols_ref, source_ref, open_ref, marks_ref, diag_ref,
    first_ref, second_ref, third_ref, rest_ref, shift_ref, fourth_ref, fifth_ref, corr_ref,
    inner_ref, expand_ref, last_ref, expands, bands,
    top, bot, lef, rig, top_corner, bot_corner, from_rows, from_cols, from_corners,
    input_sem, send_sem, recv_sem,
):
    goals, rows, cols = out_ref.shape
    tiles = cols // LANES
    rim = tiles
    span = tiles + 1
    ring = span * LANES
    wide = rows + 2 * HALO
    groups = wide // SUB
    first = SUB + HALO
    coarse_rows = wide // COARSEN
    own_coarse = rows // COARSEN
    me = (lax.axis_index("gx"), lax.axis_index("gy"))
    row_start = me[0] * rows
    col_start = me[1] * cols
    lane = lane_iota(SUB)
    sub = lax.broadcasted_iota(jnp.int32, (SUB, LANES), 0)
    zero = jnp.zeros((SUB, LANES), jnp.float32)
    coefficients = smoother_coefficients()
    inverse = 1.0 / CENTER
    natural = list(range(tiles))

    def exists(dx, dy):
        gx, gy = me[0] + dx, me[1] + dy
        return (gx >= 0) & (gx < peers[0]) & (gy >= 0) & (gy < peers[1])

    barrier = pltpu.get_barrier_semaphore()
    count = jnp.int32(0)
    for dx, dy in DIRECTIONS:
        there = exists(dx, dy)
        count = count + there.astype(jnp.int32)

        @pl.when(there)
        def _():
            pl.semaphore_signal(
                barrier, inc=1, device_id=(me[0] + dx, me[1] + dy),
                device_id_type=pl.DeviceIdType.MESH,
            )

    pairs = (
        (obst_hbm, obst_ref), (load_hbm, load_ref), (rows_hbm, exit_rows_ref),
        (cols_hbm, exit_cols_ref),
    )
    inputs = [
        pltpu.make_async_copy(there, here, input_sem.at[k]) for k, (there, here) in enumerate(pairs)
    ]
    for copied in inputs:
        copied.start()

    messages = (
        (top, from_rows.at[0]),
        (bot, from_rows.at[1]),
        (lef, from_cols.at[0]),
        (rig, from_cols.at[1]),
        (top_corner, from_corners.at[0]),
        (top.at[tiles - 1], from_corners.at[1]),
        (bot_corner, from_corners.at[2]),
        (bot.at[tiles - 1], from_corners.at[3]),
    )

    def copy(k):
        dx, dy = DIRECTIONS[k]
        return pltpu.make_async_remote_copy(
            src_ref=messages[k][0], dst_ref=messages[k][1],
            send_sem=send_sem.at[k], recv_sem=recv_sem.at[k],
            device_id=(me[0] + dx, me[1] + dy), device_id_type=pl.DeviceIdType.MESH,
        )

    def arrive(k):
        dx, dy = DIRECTIONS[k]

        @pl.when(exists(-dx, -dy))
        def _():
            copy(k).wait_recv()

    for k, (dx, dy) in enumerate(DIRECTIONS):

        @pl.when(jnp.logical_not(exists(-dx, -dy)))
        def _():
            messages[k][1][...] = jnp.zeros(messages[k][1].shape, jnp.float32)

    for ends in (0, wide + SUB):
        for t in range(span):
            open_ref[t, pl.ds(ends, SUB), :] = zero
            source_ref[t, pl.ds(ends, SUB), :] = zero
            for g in range(goals):
                for ref in (first_ref, second_ref, third_ref):
                    ref[g, t, pl.ds(ends, SUB), :] = zero

    def row(ref, at, t, *lead):
        return ref[(*lead, t, pl.ds(at, SUB), slice(None))]

    def around(ref, at, ts, *lead):
        center = [row(ref, at, t, *lead) for t in ts]
        below = [row(ref, at + 1, t, *lead) for t in ts]
        above = [row(ref, at - 1, t, *lead) for t in ts]
        up = [pltpu.roll(c, 1, 1) for c in center]
        down = [pltpu.roll(c, LANES - 1, 1) for c in center]
        total = []
        for k in range(len(ts)):
            before = jnp.where(lane == 0, up[k - 1], up[k]) if k else up[k]
            after = (
                jnp.where(lane == LANES - 1, down[k + 1], down[k]) if k + 1 < len(ts) else down[k]
            )
            total.append(below[k] + above[k] + (before + after))
        return center, total

    def inner(body, skip=0):
        low, high = EDGE + skip, groups - EDGE - skip
        size = high - low
        unroll = max(u for u in range(1, UNROLL + 1) if size % u == 0)

        def step(i, carry):
            body(i, pl.multiple_of(i * SUB + SUB, SUB), natural)
            return carry

        lax.fori_loop(low, high, step, 0, unroll=unroll)

    def over(members, ts, body):
        for i in sorted(set(members)):
            body(i, i * SUB + SUB, ts)

    early = [*range(EDGE + 1), *range(groups - EDGE - 1, groups)]
    late = [*range(EDGE - 1, 2 * EDGE), *range(groups - 2 * EDGE, groups - EDGE + 1)]
    final = [*range(EDGE, 2 * EDGE), *range(groups - 2 * EDGE, groups - EDGE)]

    def setup(i, at, ts):
        opened, open_around = around(open_ref, at, ts)
        source, source_around = around(source_ref, at, ts)
        for k, t in enumerate(ts):
            base = (1.0 - inverse * (SCREENING + 4.0)) + opened[k] * (
                4.0 * inverse - inverse * open_around[k]
            )
            mixed = (coefficients[3] * inverse) * opened[k] * source_around[k]
            mixed = mixed + coefficients[2] * source[k]
            lifted = coefficients[3] * source[k]
            for g in range(goals):
                kept = base + opened[k] * row(marks_ref, at, t, g)
                diag_ref[g, t, pl.ds(at, SUB), :] = kept
                first_ref[g, t, pl.ds(at, SUB), :] = kept * lifted + mixed

    def horner(old_ref, new_ref, coefficient, rhs):
        def body(i, at, ts):
            weight = [inverse * row(open_ref, at, t) for t in ts]
            for g in range(goals):
                center, total = around(old_ref, at, ts, g)
                for k, t in enumerate(ts):
                    kept = row(diag_ref, at, t, g)
                    new_ref[g, t, pl.ds(at, SUB), :] = (
                        kept * center[k] + weight[k] * total[k] + coefficient * rhs(g, t, at)
                    )

        return body

    plain = lambda g, t, at: row(source_ref, at, t)
    shifted = lambda g, t, at: row(shift_ref, at, t, g)
    second = horner(first_ref, second_ref, coefficients[1], plain)
    third = horner(second_ref, third_ref, coefficients[0], plain)
    fifth = horner(fourth_ref, fifth_ref, coefficients[1], shifted)

    def residual(i, at, ts):
        opened = [row(open_ref, at, t) for t in ts]
        for g in range(goals):
            center, total = around(third_ref, at, ts, g)
            for k, t in enumerate(ts):
                kept = CENTER * (row(diag_ref, at, t, g) - 1.0)
                rest_ref[g, t, pl.ds(at, SUB), :] = (
                    row(source_ref, at, t) + kept * center[k] + opened[k] * total[k]
                )

    def spread(ref, at, t, *lead):
        even = jnp.broadcast_to(ref[(*lead, t, pl.ds(at, 1), slice(None))], (SUB, LANES))
        odd = jnp.broadcast_to(ref[(*lead, t, pl.ds(at + 1, 1), slice(None))], (SUB, LANES))
        return jnp.where(sub < COARSEN, even, odd)

    def corrections(ref, skip):
        def body(i, at, ts):
            for t in ts:
                corr_ref[t, pl.ds(at, SUB), :] = row(open_ref, at, t) * spread(ref, 2 * (i - skip), t)

        return body

    def shift(i, at, ts):
        opened = [row(open_ref, at, t) for t in ts]
        center, total = around(corr_ref, at, ts)
        moved = [opened[k] * total[k] for k in range(len(ts))]
        for g in range(goals):
            for k, t in enumerate(ts):
                kept = CENTER * (row(diag_ref, at, t, g) - 1.0)
                shift_ref[g, t, pl.ds(at, SUB), :] = (
                    row(rest_ref, at, t, g) + kept * center[k] + moved[k]
                )

    def fourth(i, at, ts):
        weight = [(coefficients[3] * inverse) * row(open_ref, at, t) for t in ts]
        for g in range(goals):
            center, total = around(shift_ref, at, ts, g)
            for k, t in enumerate(ts):
                kept = row(diag_ref, at, t, g)
                fourth_ref[g, t, pl.ds(at, SUB), :] = (
                    (coefficients[3] * kept + coefficients[2]) * center[k] + weight[k] * total[k]
                )

    def result(put):
        def body(i, at, ts):
            weight = [inverse * row(open_ref, at, t) for t in ts]
            for g in range(goals):
                center, total = around(fifth_ref, at, ts, g)
                for k, t in enumerate(ts):
                    put(
                        g, t, at - first,
                        row(third_ref, at, t, g) + row(corr_ref, at, t)
                        + row(diag_ref, at, t, g) * center[k] + weight[k] * total[k]
                        + coefficients[0] * row(shift_ref, at, t, g),
                    )

        return body

    def put(g, t, at, value):
        start = at if isinstance(at, int) else pl.multiple_of(at, SUB)
        out_ref[g, pl.ds(start, SUB), pl.ds(t * LANES, LANES)] = value

    def put_rim(g, t, at, value):
        left = (g, pl.ds(at, SUB), pl.ds(0, LANES))
        out_ref[left] = jnp.where(lane < HALO, value, out_ref[left])
        fourth_ref[g, t, pl.ds(at, SUB), :] = value

    position = lax.broadcasted_iota(jnp.int32, (ring, LANES), 0)
    rim_lane = position - cols
    fine = jnp.where(
        position < cols + LEFT_OWN,
        jnp.where(position < cols, position, rim_lane),
        jnp.where(
            rim_lane < RIGHT_HALO + HALO,
            rim_lane + (cols - RIGHT_HALO), rim_lane + (COARSEN - 1) * LANES,
        ),
    ) // COARSEN
    member = (rim_lane < RIGHT_HALO + HALO) | (rim_lane >= LANES - HALO)
    trusted = ((position >= HALO) & (position < cols - HALO)) | (
        (rim_lane >= 0) & ((rim_lane < HALO) | ((rim_lane >= RIGHT_HALO - HALO) & member))
    )
    same = fine == lax.broadcasted_iota(jnp.int32, (ring, LANES), 1)
    expands[...] = jnp.where(same & member, 1.0, 0.0).astype(jnp.bfloat16)
    restricts = jnp.where(same & trusted, 1.0, 0.0).astype(jnp.bfloat16)

    def coarse_column(axis):
        at = lax.broadcasted_iota(jnp.int32, (LANES, LANES), axis)
        at = jnp.where(at < cols // COARSEN + LANES // 8, at, at - LANES) + col_start // COARSEN
        return at, (at >= 0) & (at < peers[1] * cols // COARSEN)

    (from_col, from_floor), (to_col, to_floor) = coarse_column(0), coarse_column(1)
    touches = ((from_col == to_col + 1) | (from_col == to_col - 1)) & from_floor & to_floor
    step = jnp.where(touches, 1.0, 0.0).astype(jnp.bfloat16)
    bands[:, pl.ds(0, LANES)] = restricts
    walk = restricts
    for k in range(1, CSWEEPS):
        walk = jnp.dot(walk, step, preferred_element_type=jnp.float32).astype(jnp.bfloat16)
        bands[:, pl.ds(k * LANES, LANES)] = walk

    def product(value, matrix, dims):
        high = value.astype(jnp.bfloat16)
        low = (value - high.astype(jnp.float32)).astype(jnp.bfloat16)
        both = lax.dot_general(
            jnp.concatenate([high, low], axis=0), matrix, (dims, ((), ())),
            preferred_element_type=jnp.float32,
        )
        size = value.shape[0]
        return both[:size] + both[size:]

    def restrict(ref, offset, size, ts, matrix, leads):
        stacked = []
        for t in ts:
            blocks = []
            for lead in leads:
                part = [
                    ref[(*lead, t, pl.ds(offset + k, size, stride=COARSEN), slice(None))]
                    for k in range(COARSEN)
                ]
                blocks.append((part[0] + part[1]) + (part[2] + part[3]))
            stacked.append(jnp.concatenate(blocks, axis=0) if len(blocks) > 1 else blocks[0])
        return product(jnp.concatenate(stacked, axis=1), matrix, ((1,), (0,)))

    shape = (coarse_rows, LANES)
    coarse_row = lax.broadcasted_iota(jnp.int32, shape, 0) - COARSE_HALO + row_start // COARSEN
    floor = ((coarse_row >= 0) & (coarse_row < peers[0] * rows // COARSEN)).astype(jnp.float32)
    powers = coarse_coefficients()

    def coarse_solve(walks, inside):
        size = walks.shape[0]
        walks = [walks[:, k * LANES : (k + 1) * LANES] for k in range(CSWEEPS)]
        estimate = None
        for j in reversed(range(CSWEEPS)):
            part = powers[j] * walks[0]
            for k in range(j + 1, CSWEEPS):
                part = part + (powers[k] * math.comb(k, j)) * walks[k - j]
            if estimate is not None:
                near = pltpu.roll(estimate, size - 1, 0) + pltpu.roll(estimate, 1, 0)
                part = part + (near if inside is None else near * inside)
            estimate = part
        return estimate

    for copied in inputs:
        copied.wait()

    def blend(i, at):
        for t in natural:
            block = (pl.ds(at, SUB), pl.ds(t * LANES, LANES))
            opened = (1 - obst_ref[block]).astype(jnp.float32)
            into = (t, pl.ds(at + first, SUB), slice(None))
            open_ref[into] = opened
            source_ref[into] = opened * load_ref[block]

    for at in range(0, rows, SUB):
        blend(at, at)

    def mixed_rim(left_tile, right_tile):
        turned = pltpu.roll(right_tile, RIGHT_HALO, 1)
        return jnp.where(lane < LEFT_OWN, left_tile, jnp.where(lane < RIGHT_HALO, turned, 0.0))

    for t in natural:
        top[t] = source_ref[t, pl.ds(first, HALO), :]
        bot[t] = source_ref[t, pl.ds(first + rows - HALO, HALO), :]
    top_corner[...] = pltpu.roll(source_ref[0, pl.ds(first, HALO), :], RIGHT_HALO, 1)
    bot_corner[...] = pltpu.roll(source_ref[0, pl.ds(first + rows - HALO, HALO), :], RIGHT_HALO, 1)
    tall = lane_iota(HALO)
    block = LANES // HALO
    for pack in range(rows // LANES):
        left = jnp.zeros((HALO, LANES), jnp.float32)
        right = jnp.zeros((HALO, LANES), jnp.float32)
        for b in range(block):
            start = first + pack * LANES + b * HALO
            here = (tall >= b * HALO) & (tall < (b + 1) * HALO)
            low = source_ref[0, pl.ds(start, HALO), :]
            high = source_ref[tiles - 1, pl.ds(start, HALO), :]
            left = jnp.where(here, pltpu.roll(low, b * HALO, 1) if b else low, left)
            turn = ((b + 1) * HALO) % LANES
            right = jnp.where(here, pltpu.roll(high, turn, 1) if turn else high, right)
        lef[pl.ds(pack * HALO, HALO), :] = left
        rig[pl.ds(pack * HALO, HALO), :] = right
    for i in range(EDGE, groups - EDGE):
        at = i * SUB + SUB
        source_ref[rim, pl.ds(at, SUB), :] = mixed_rim(
            row(source_ref, at, 0), row(source_ref, at, tiles - 1)
        )

    exits = exit_rows_ref.shape[1]
    row_of = lax.broadcasted_iota(jnp.int32, (wide, exits), 0) + (row_start - HALO)
    spot = lax.broadcasted_iota(jnp.int32, (ring, exits), 0)
    col_of = jnp.where(
        spot < cols, spot,
        jnp.where(
            spot < cols + LEFT_OWN, spot - cols,
            jnp.where(spot < cols + RIGHT_HALO + HALO, spot - RIGHT_HALO, spot - (cols + LANES)),
        ),
    ) + col_start
    for g in range(goals):
        row_hot = (row_of == exit_rows_ref[pl.ds(g, 1), :]).astype(jnp.float32)
        col_hot = (col_of == exit_cols_ref[pl.ds(g, 1), :]).astype(jnp.float32)
        marks = lax.dot_general(
            row_hot.astype(jnp.bfloat16), col_hot.astype(jnp.bfloat16),
            (((1,), (1,)), ((), ())), preferred_element_type=jnp.float32,
        )
        marks = jnp.minimum(marks, 1.0) * (-EXIT_SINK * inverse)
        for t in range(span):
            marks_ref[g, t, pl.ds(SUB, wide), :] = marks[:, t * LANES : (t + 1) * LANES]

    def part_one():
        inner(setup)
        inner(second)

    def part_two():
        inner(third)
        inner(residual)
        walk = expands[:cols, :]
        inner_bands = [walk]
        for k in range(1, CSWEEPS):
            walk = jnp.dot(walk, step, preferred_element_type=jnp.float32).astype(jnp.bfloat16)
            inner_bands.append(walk)
        inner_bands = jnp.concatenate(inner_bands, axis=1)
        known = coarse_solve(
            restrict(source_ref, first, own_coarse, natural, inner_bands, [()]), None
        )
        columns = product(known, expands[:cols, :], ((1,), (1,)))
        for t in natural:
            inner_ref[t] = columns[:, t * LANES : (t + 1) * LANES]
        inner(corrections(inner_ref, EDGE))
        inner(shift, EDGE - 1)
        inner(fourth, EDGE - 1)
        inner(fifth, EDGE - 1)
        inner(result(put), EDGE)

    part_one()

    pl.semaphore_wait(barrier, count)
    order = (4, 5, 6, 7, 2, 3, 0, 1)
    for k in order:

        @pl.when(exists(*DIRECTIONS[k]))
        def _():
            copy(k).start()

    part_two()

    arrive(0)
    arrive(1)
    for t in natural:
        for here, ref in ((first + rows, from_rows.at[0, t]), (SUB, from_rows.at[1, t])):
            for b in range(EDGE):
                value = ref[pl.ds(b * SUB, SUB), :]
                source_ref[t, pl.ds(here + b * SUB, SUB), :] = value
                open_ref[t, pl.ds(here + b * SUB, SUB), :] = (value > 0.0).astype(jnp.float32)
    over(early, natural, setup)
    over(early, natural, second)
    over(early, natural, third)
    over(early, natural, residual)

    arrive(2)
    arrive(3)

    is_right = (lane >= RIGHT_HALO) & (lane < RIGHT_HALO + HALO)
    is_left = lane >= LANES - HALO

    def set_rim(at, value):
        source_ref[rim, pl.ds(at, SUB), :] = value
        open_ref[rim, pl.ds(at, SUB), :] = (value > 0.0).astype(jnp.float32)

    for pack in range(rows // LANES):
        for b in range(block):
            for c in range(EDGE):
                part = pl.ds(pack * HALO + c * SUB, SUB)
                right = pltpu.roll(from_cols[0, part, :], (RIGHT_HALO - b * HALO) % LANES, 1)
                left = from_cols[1, part, :]
                turn = (LANES - HALO - b * HALO) % LANES
                left = pltpu.roll(left, turn, 1) if turn else left
                at = first + pack * LANES + b * HALO + c * SUB
                value = jnp.where(is_right, right, row(source_ref, at, rim))
                set_rim(at, jnp.where(is_left, left, value))

    tall_rim, short_rim, own_rim = (range(k, groups - k) for k in (0, EDGE - 1, EDGE))
    ahead = [range(k, groups - k) for k in (EDGE + 1, EDGE + 2)]
    over(ahead[0], [rim], setup)
    over(ahead[1], [rim], second)

    for k in (4, 5, 6, 7):
        arrive(k)

    for side, here in ((0, first + rows), (1, SUB)):
        for b in range(EDGE):
            at = here + b * SUB
            part = pl.ds(b * SUB, SUB)
            base = mixed_rim(row(source_ref, at, 0), row(source_ref, at, tiles - 1))
            value = jnp.where(is_right, from_corners[2 * side, part, :], base)
            set_rim(at, jnp.where(is_left, from_corners[2 * side + 1, part, :], value))
    everything = list(range(span))
    known = coarse_solve(restrict(source_ref, SUB, coarse_rows, everything, bands[...], [()]), floor)
    columns = product(known, expands[...], ((1,), (1,)))
    for t in everything:
        expand_ref[t] = columns[:, t * LANES : (t + 1) * LANES]

    over(set(tall_rim) - set(ahead[0]), [rim], setup)
    over(set(tall_rim) - set(ahead[1]), [rim], second)
    over(tall_rim, [rim], third)
    over(tall_rim, [rim], residual)

    leads = [(g,) for g in range(goals)]
    estimates = coarse_solve(
        restrict(rest_ref, SUB, coarse_rows, everything, bands[...], leads),
        jnp.concatenate([floor] * goals, axis=0),
    )
    columns = product(estimates, expands[:cols, :], ((1,), (1,)))
    for g in range(goals):
        for t in natural:
            last_ref[g, t] = columns[
                g * coarse_rows : (g + 1) * coarse_rows, t * LANES : (t + 1) * LANES
            ]

    for ts, members in (([rim], short_rim), (natural, late)):
        over(members, ts, corrections(expand_ref, 0))
    for body in (shift, fourth, fifth):
        for ts, members in (([rim], short_rim), (natural, late)):
            over(members, ts, body)
    over(final, natural, result(put))
    over(own_rim, [rim], result(put_rim))
    for i in range(EDGE, groups - EDGE):
        at = i * SUB + SUB - first
        for g in range(goals):
            right = (g, pl.ds(at, SUB), pl.ds(cols - LANES, LANES))
            turned = pltpu.roll(row(fourth_ref, at, rim, g), LANES - RIGHT_HALO, 1)
            out_ref[right] = jnp.where(lane >= LANES - HALO, turned, out_ref[right])

    for i in range(EDGE, groups - EDGE):
        at = i * SUB + SUB
        opened = [row(open_ref, at, t) for t in natural]
        for g in range(goals):
            for t in natural:
                block = (g, pl.ds(at - first, SUB), pl.ds(t * LANES, LANES))
                out_ref[block] = out_ref[block] + opened[t] * spread(last_ref, 2 * i, t, g)

    for k in order:

        @pl.when(exists(*DIRECTIONS[k]))
        def _():
            copy(k).wait_send()


def per_device(peers, obstacles, load, exit_rows, exit_cols):
    rows, cols = obstacles.shape
    goals = exit_rows.shape[0]
    tiles = cols // LANES
    span = tiles + 1
    wide = rows + 2 * HALO
    padded = wide + 2 * SUB
    f32 = jnp.float32
    vmem = pl.BlockSpec(memory_space=pltpu.VMEM)
    packed = rows * HALO // LANES
    exits = exit_rows.shape
    field = pltpu.VMEM((goals, span, padded, LANES), f32)
    shared = pltpu.VMEM((span, padded, LANES), f32)
    coarse = wide // COARSEN
    strip = pltpu.VMEM((tiles, HALO, LANES), f32)
    column = pltpu.VMEM((packed, LANES), f32)
    corner = pltpu.VMEM((HALO, LANES), f32)
    return pl.pallas_call(
        functools.partial(cycles_kernel, peers),
        out_shape=jax.ShapeDtypeStruct((goals, rows, cols), f32),
        in_specs=[pl.BlockSpec(memory_space=pltpu.HBM)] * 4,
        out_specs=vmem,
        scratch_shapes=[
            pltpu.VMEM((rows, cols), jnp.int32),
            pltpu.VMEM((rows, cols), f32),
            pltpu.VMEM(exits, jnp.int32),
            pltpu.VMEM(exits, jnp.int32),
            shared, shared, field, field,
            field, field, field, field, field, field, field, shared,
            pltpu.VMEM((tiles, rows // COARSEN, LANES), f32),
            pltpu.VMEM((span, coarse, LANES), f32),
            pltpu.VMEM((goals, tiles, coarse, LANES), f32),
            pltpu.VMEM((span * LANES, LANES), jnp.bfloat16),
            pltpu.VMEM((span * LANES, CSWEEPS * LANES), jnp.bfloat16),
            strip, strip, column, column, corner, corner,
            pltpu.VMEM((2, tiles, HALO, LANES), f32),
            pltpu.VMEM((2, packed, LANES), f32),
            pltpu.VMEM((4, HALO, LANES), f32),
            pltpu.SemaphoreType.DMA((4,)),
            pltpu.SemaphoreType.DMA((len(DIRECTIONS),)),
            pltpu.SemaphoreType.DMA((len(DIRECTIONS),)),
        ],
        compiler_params=pltpu.CompilerParams(
            collective_id=0, has_side_effects=True, vmem_limit_bytes=48 * 1024 * 1024
        ),
        name="cycles",
    )(*(pltpu.with_memory_space_constraint(x, pltpu.HBM) for x in (obstacles, load, exit_rows, exit_cols)))


def solution(mesh):
    peers = (mesh.shape["gx"], mesh.shape["gy"])
    return jax.shard_map(
        functools.partial(per_device, peers),
        mesh=mesh,
        in_specs=(P("gx", "gy"), P("gx", "gy"), P(), P()),
        out_specs=P(None, "gx", "gy"),
        check_vma=False,
    )
```
